1024 devices in a mesh: dom: 64 (over z, y), grp: 16 (over x, core).
Axes of the slice: x: 8, y: 8, z: 8, core: 2. Of those that a mesh axis runs over, the one named last changes fastest.
Arguments:
- old_state: float32 [9, 56, 131072], P(None, None, ('dom', 'grp')), may hold values from -6 to 6
- stiffness: float32 [3, 56, 56], replicated, may hold values from -0.75 to 0.75
- jacobians: float32 [3, 9, 9, 131072], P(None, None, None, ('dom', 'grp')), may hold values from -2 to 2
- lift_own: float32 [4, 56, 56], replicated, may hold values from -0.75 to 0.75
- lift_across: float32 [4, 4, 56, 56], replicated, may hold values from -0.75 to 0.75
- riemann: float32 [2, 4, 9, 9, 131072], P(None, None, None, None, ('dom', 'grp')), may hold values from -2 to 2
- cluster_ids: int32 [131072], P(('dom', 'grp')), may hold values from 0 to 2
- send_slots: int32 [327680], P(('dom', 'grp')), may hold values from 0 to 127, as said below
- face_partner: int32 [4, 131072], P(None, ('dom', 'grp')), may hold values from 0 to 447, as said below
- partner_face: int32 [4, 131072], P(None, ('dom', 'grp')), may hold values from 0 to 3
- cohesion: float32 [131072], P(('dom', 'grp')), may hold values from 1 to 4
- relax_time: float32 [131072], P(('dom', 'grp')), may hold values from 0.1 to 1
- yield_flag: int32 [131072], P(('dom', 'grp')), may hold values 0 or 1
Outputs:
- new_state: float32 [9, 56, 131072], P(None, None, ('dom', 'grp'))
The draws below stay inside these ranges and needn't reach their ends.
Inputs may be any that keep to these rules, and one draw needn't show every extreme that they name: `send_slots`: local element numbers of the sending device; its first 256 slots go in equal shares to the devices of its grp group in grp order, the next 32 to the device one index lower along dom and the last 32 to the one one index higher, cyclically; the slots bound for one destination name distinct elements. `face_partner`: a place of the device's neighbour list: own elements, then what the grp group sends it, sender by sender, then what the lower and the higher dom neighbour send it; every received place is the partner of exactly one face of the device, all other faces have own places.
All inputs are finite; a program needn't handle non-finite values. No bound on the sum of `yield_flag` on one device may be relied on, other than what follows from the above.
Results may differ from the reference program's by a relative error of at most 0.0003.
Values sent between devices are 32-bit elements; how exact they have to be, the bound alone decides.
A program may use at most 64 MiB of HBM per device.

```python
import math
import jax
import jax.numpy as jnp
from jax import lax

QUANT = 9
MODES = 56
ORDER = 6
ELEM_DEV = 128
GRP_SLOTS = 256
HALO = 32
ELEMS = 131072
SENDS = 327680
N_DOM = 64
N_GRP = 16


def distinct_orders(key, leading, count):
    scores = jax.random.randint(key, leading + (count,), 0, 1048576, dtype=jnp.int32)
    scores = scores * count + jnp.arange(count, dtype=jnp.int32)
    return jnp.argsort(scores, axis=-1).astype(jnp.int32)


def draw_send_slots(key, part):
    device_total = ELEMS // ELEM_DEV
    share = GRP_SLOTS // N_GRP
    peer_orders = distinct_orders(jax.random.fold_in(key, 11), (device_total, N_GRP), ELEM_DEV)
    peer_part = peer_orders[:, :, :share].reshape(device_total, GRP_SLOTS)
    lower_orders = distinct_orders(jax.random.fold_in(key, 12), (device_total,), ELEM_DEV)
    upper_orders = distinct_orders(jax.random.fold_in(key, 13), (device_total,), ELEM_DEV)
    whole = jnp.concatenate([peer_part, lower_orders[:, :HALO], upper_orders[:, :HALO]], axis=1)
    return whole.reshape(SENDS).astype(jnp.int32)


def draw_face_partner(key, part):
    device_total = ELEMS // ELEM_DEV
    faces = 4 * ELEM_DEV
    received = GRP_SLOTS + 2 * HALO
    order = distinct_orders(jax.random.fold_in(key, 21), (device_total,), faces)
    rank = jnp.argsort(order, axis=-1).astype(jnp.int32)
    local = jax.random.randint(jax.random.fold_in(key, 22), (device_total, faces), 0, ELEM_DEV, dtype=jnp.int32)
    places = jnp.where(rank < received, ELEM_DEV + rank, local)
    places = places.reshape(device_total, 4, ELEM_DEV)
    return jnp.transpose(places, (1, 0, 2)).reshape(4, ELEMS).astype(jnp.int32)


def with_ends(drawn, rng, least, largest):
    spot = [jax.random.randint(jax.random.fold_in(rng, axis), (), 0, length) for axis, length in enumerate(drawn.shape)]
    longest = drawn.shape.index(max(drawn.shape))
    beside = spot[:longest] + [(spot[longest] + 1) % drawn.shape[longest]] + spot[longest + 1:]
    return drawn.at[tuple(spot)].set(least).at[tuple(beside)].set(largest)


def steps_of(own_key, extent, cuts, smallest, high):
    factor_of = 1.0
    for position, parts in cuts:
        heights = jax.random.uniform(jax.random.fold_in(jax.random.fold_in(own_key, 6), position), (parts,), jnp.float32, smallest / len(cuts), high / len(cuts))
        factor_of = factor_of * jnp.repeat(jnp.exp(heights), extent[position] // parts).reshape((-1,) + (1,) * (len(extent) - 1 - position))
    return factor_of


def gaussian(key, shape, scale, most, split=(), kind=jnp.bfloat16):
    result = scale * jax.random.normal(key, shape, jnp.float32)
    if split:
        result = result * steps_of(key, shape, split, -0.22, 0.18)
    return jnp.clip(result, -most, most).astype(kind)


def setup_inputs(seed: int = 0) -> dict:
    key_of = jax.random.split(jax.random.key(seed), 14)
    return {
        "old_state": gaussian(key_of[0], (QUANT, MODES, ELEMS), 1.0, 6.0, ((2, 1024),), jnp.float32),
        "stiffness": gaussian(key_of[1], (3, MODES, MODES), MODES ** -0.5, 0.75, (), jnp.float32),
        "jacobians": gaussian(key_of[2], (3, QUANT, QUANT, ELEMS), QUANT ** -0.5, 2.0, ((3, 1024),), jnp.float32),
        "lift_own": gaussian(key_of[3], (4, MODES, MODES), MODES ** -0.5, 0.75, (), jnp.float32),
        "lift_across": gaussian(key_of[4], (4, 4, MODES, MODES), MODES ** -0.5, 0.75, (), jnp.float32),
        "riemann": gaussian(key_of[5], (2, 4, QUANT, QUANT, ELEMS), QUANT ** -0.5, 2.0, ((4, 1024),), jnp.float32),
        "cluster_ids": with_ends(jax.random.randint(key_of[6], (ELEMS,), 0, 3), jax.random.fold_in(key_of[6], 1), 0, 2).astype(jnp.int32),
        "send_slots": draw_send_slots(jax.random.fold_in(key_of[13], 71), 0),
        "face_partner": draw_face_partner(jax.random.fold_in(key_of[13], 71), 0),
        "partner_face": with_ends(jax.random.randint(key_of[9], (4, ELEMS), 0, 4), jax.random.fold_in(key_of[9], 1), 0, 3).astype(jnp.int32),
        "cohesion": jnp.clip(1.0 + 3.0 * jax.random.uniform(key_of[10], (ELEMS,), jnp.float32) ** steps_of(key_of[10], (ELEMS,), ((0, 1024),), -0.2, 0.2), 1.0, 4.0),
        "relax_time": jnp.clip(jnp.exp(math.log(1.0) - 2.3025851 * jax.random.uniform(key_of[11], (ELEMS,), jnp.float32) ** steps_of(key_of[11], (ELEMS,), ((0, 1024),), -0.2, 0.2)), 0.1, 1.0),
        "yield_flag": with_ends((jax.random.randint(key_of[12], (ELEMS,), 0, 2) < 1).astype(jnp.int32), jax.random.fold_in(key_of[12], 1), 0, 1),
    }


base_step = 0.2
highest = lax.Precision.HIGHEST

def step_table(terms_count):
    entries = []
    for rate_level in range(3):
        interval = base_step * 2.0 ** rate_level
        factorial = 1.0
        powers = []
        for degree in range(terms_count):
            factorial = factorial * (degree + 1)
            powers.append(interval ** (degree + 1) / factorial)
        entries.append(powers)
    return jnp.array(entries, dtype=jnp.float32)

def clock_steps():
    return jnp.array([base_step, 2.0 * base_step, 4.0 * base_step], dtype=jnp.float32)

def cluster_selector(cluster_ids):
    return (cluster_ids[None, :] == jnp.arange(3, dtype=jnp.int32)[:, None]).astype(jnp.float32)

def on_modes(matrix, operand):
    return jnp.einsum('mn,qne->qme', matrix, operand, precision=highest)

def on_quantities(operand, blocks):
    return lax.optimization_barrier(jnp.sum(operand[:, None, :, :] * blocks[:, :, None, :], axis=0))

def taylor_stack(initial, stiffness, jacobian):
    collected = [initial]
    for degree in range(1, ORDER):
        latest = collected[-1]
        change = on_quantities(on_modes(stiffness[0], latest), jacobian[0])
        change = change + on_quantities(on_modes(stiffness[1], latest), jacobian[1])
        change = change + on_quantities(on_modes(stiffness[2], latest), jacobian[2])
        collected.append(-change)
    return jnp.stack(collected)

def integrate(stacked, weights):
    summed = weights[0] * stacked[0]
    for degree in range(1, stacked.shape[0]):
        summed = summed + weights[degree] * stacked[degree]
    return summed

def volume_term(own_int, stiffness, jacobian):
    summed = on_modes(stiffness[0].T, on_quantities(own_int, jacobian[0]))
    summed = summed + on_modes(stiffness[1].T, on_quantities(own_int, jacobian[1]))
    summed = summed + on_modes(stiffness[2].T, on_quantities(own_int, jacobian[2]))
    return summed

def face_update(own_int, neighbours, partner_sides, lift_own, lift_across, riemann):
    summed = jnp.zeros_like(own_int)
    candidates = jnp.arange(4, dtype=jnp.int32)[:, None]
    for face_index in range(4):
        summed = summed + on_quantities(on_modes(lift_own[face_index], own_int), riemann[0, face_index])
        projected = jnp.einsum('jmn,qne->qjme', lift_across[face_index], neighbours[face_index], precision=highest)
        picker = (partner_sides[face_index][None, :] == candidates).astype(jnp.float32)
        chosen = lax.optimization_barrier(jnp.sum(projected * picker[None, :, None, :], axis=1))
        summed = summed + on_quantities(chosen, riemann[1, face_index])
    return summed

def plastic(updated, cohesion, relax_time, yielding, interval):
    isotropic = (jnp.arange(6, dtype=jnp.int32) < 3).astype(jnp.float32)[:, None, None]
    pressure = (updated[0] + updated[1] + updated[2]) / 3.0
    deviator = updated[:6] - isotropic * pressure[None]
    centre = deviator[:, 0, :]
    second = 0.5 * (centre[0] * centre[0] + centre[1] * centre[1] + centre[2] * centre[2])
    second = second + centre[3] * centre[3] + centre[4] * centre[4] + centre[5] * centre[5]
    strength = jnp.sqrt(second)
    excess = jnp.maximum(strength - cohesion, 0.0) / jnp.maximum(strength, cohesion)
    factor = yielding.astype(jnp.float32) * excess * (1.0 - jnp.exp(-interval / relax_time))
    return jnp.concatenate([updated[:6] - factor[None, None, :] * deviator, updated[6:]], axis=0)

def advance(own_block, stiffness, jacobian, lift_own, lift_across, riemann, selector, own_int, neighbours, partner_sides, cohesion, relax_time, yielding):
    updated = own_block + volume_term(own_int, stiffness, jacobian)
    updated = updated - face_update(own_int, neighbours, partner_sides, lift_own, lift_across, riemann)
    interval = lax.optimization_barrier(jnp.sum(selector * clock_steps()[:, None], axis=0))
    return plastic(updated, cohesion, relax_time, yielding, interval)

def reference(old_state, stiffness, jacobians, lift_own, lift_across, riemann, cluster_ids, send_slots, face_partner, partner_face, cohesion, relax_time, yield_flag):
    device_total = N_DOM * N_GRP
    per_device = ELEM_DEV
    peer_slots = GRP_SLOTS // N_GRP
    sent_count = GRP_SLOTS + 2 * HALO
    taylor_table = step_table(ORDER)
    sends = send_slots.reshape(device_total, sent_count)

    def predict(device):
        offset = (device * per_device).astype(jnp.int32)
        own_block = lax.dynamic_slice_in_dim(old_state, offset, per_device, 2)
        jacobian = lax.dynamic_slice_in_dim(jacobians, offset, per_device, 3)
        collected = taylor_stack(own_block, stiffness, jacobian)
        return jnp.stack([integrate(collected, taylor_table[rate_level][:, None]) for rate_level in range(3)])
    device_ids = jnp.arange(device_total, dtype=jnp.int32)
    levels = lax.map(predict, device_ids)

    def update(device):
        offset = (device * per_device).astype(jnp.int32)
        dom_index = device // N_GRP
        grp_index = device % N_GRP
        peer_ids = dom_index * N_GRP + jnp.arange(N_GRP, dtype=jnp.int32)
        peer_devices = jnp.repeat(peer_ids, peer_slots)
        peer_columns = grp_index * peer_slots + jnp.tile(jnp.arange(peer_slots, dtype=jnp.int32), N_GRP)
        peer_elements = sends[peer_devices, peer_columns]
        below = (dom_index + N_DOM - 1) % N_DOM * N_GRP + grp_index
        above = (dom_index + 1) % N_DOM * N_GRP + grp_index
        rim_range = jnp.arange(HALO, dtype=jnp.int32)
        below_elements = sends[below, GRP_SLOTS + HALO + rim_range]
        above_elements = sends[above, GRP_SLOTS + rim_range]
        source_device = jnp.concatenate([jnp.full((per_device,), device, jnp.int32), peer_devices, jnp.full((HALO,), below, jnp.int32), jnp.full((HALO,), above, jnp.int32)])
        source_element = jnp.concatenate([jnp.arange(per_device, dtype=jnp.int32), peer_elements, below_elements, above_elements])
        own_clusters = lax.dynamic_slice_in_dim(cluster_ids, offset, per_device, 0)
        selector = cluster_selector(own_clusters)
        own_int = lax.optimization_barrier(jnp.sum(levels[device] * selector[:, None, None, :], axis=0))
        partners = lax.dynamic_slice_in_dim(face_partner, offset, per_device, 1)
        partner_sides = lax.dynamic_slice_in_dim(partner_face, offset, per_device, 1)
        neighbours = []
        for face_index in range(4):
            owner_ids = source_device[partners[face_index]]
            element_ids = source_element[partners[face_index]]
            picked = jnp.transpose(levels[owner_ids, :, :, :, element_ids], (1, 2, 3, 0))
            neighbours.append(lax.optimization_barrier(jnp.sum(picked * selector[:, None, None, :], axis=0)))
        own_block = lax.dynamic_slice_in_dim(old_state, offset, per_device, 2)
        jacobian = lax.dynamic_slice_in_dim(jacobians, offset, per_device, 3)
        solvers = lax.dynamic_slice_in_dim(riemann, offset, per_device, 4)
        return advance(own_block, stiffness, jacobian, lift_own, lift_across, solvers, selector, own_int, neighbours, partner_sides, lax.dynamic_slice_in_dim(cohesion, offset, per_device, 0), lax.dynamic_slice_in_dim(relax_time, offset, per_device, 0), lax.dynamic_slice_in_dim(yield_flag, offset, per_device, 0))
    results = lax.map(update, device_ids)
    return jnp.transpose(results, (1, 2, 0, 3)).reshape(QUANT, MODES, ELEMS)
```

```python
import jax
import jax.numpy as jnp
from jax import lax
from jax.experimental import pallas as pl
from jax.experimental.pallas import tpu as pltpu
from jax.sharding import PartitionSpec as P

QUANT = 9
MODES = 56
ORDER = 6
ELEM = 128
GRP_SLOTS = 256
HALO = 32
N_GRP = 16
SHARE = GRP_SLOTS // N_GRP
CHIPS = N_GRP // 2
ROWS = QUANT * MODES
WIRE = 512
MESH = pl.DeviceIdType.MESH
F32 = jnp.float32
base_step = 0.2

PEERS = tuple(
    (d % CHIPS, c)
    for d in (4, 3, -3, 2, -2, 1, -1, 0)
    for c in (0, 1)
    if (d, c) != (0, 0)
)
N_PEERS = len(PEERS)
GROUPS = ((0, 32), (32, 24))


def taylor_table():
    entries = []
    for rate_level in range(3):
        interval = base_step * 2.0**rate_level
        factorial = 1.0
        powers = []
        for degree in range(ORDER):
            factorial = factorial * (degree + 1)
            powers.append(interval ** (degree + 1) / factorial)
        entries.append(powers)
    return entries


TABLE = taylor_table()


def split(x):
    hi = x.astype(jnp.bfloat16).astype(F32)
    return hi, x - hi


def dot(a, b):
    return lax.dot_general(a, b, (((1,), (0,)), ((), ())), preferred_element_type=F32)


def dot_nt(a, b):
    return lax.dot_general(a, b, (((1,), (1,)), ((), ())), preferred_element_type=F32)


def stack_weights(w, dst, rows):
    hi, lo = split(w)
    dst[rows, 0:128] = hi + pltpu.roll(hi, 64, 1)
    dst[rows, 128:256] = lo


def store_operand(rs, q, r0, rn, x):
    hi, lo = split(x)
    lanes = pl.ds(q * 128, 128)
    rs[pl.ds(r0, rn), lanes] = hi
    rs[pl.ds(64 + r0, rn), lanes] = lo
    rs[pl.ds(128 + r0, rn), lanes] = hi


def apply_modes(w, rs, kx, rows):
    for j in range(5):
        if j < 4:
            out = dot(w, rs[:, 256 * j : 256 * j + 256])
            kx[2 * j, 0:rows, :] = out[:, 0:128]
            kx[2 * j + 1, 0:rows, :] = out[:, 128:256]
        else:
            kx[8, 0:rows, :] = dot(w, rs[:, 1024:1152])


def kernel(
    old,
    stiff,
    jac,
    lown,
    lacross,
    riem,
    cluster,
    slots,
    fpart,
    pface,
    cohesion,
    relax_time,
    yflag,
    out,
    rs,
    kx,
    sb,
    wpad,
    wk,
    wown,
    wx,
    qm,
    lev,
    lv,
    near,
    upd,
    send,
    recv,
    rq_send,
    rq_recv,
    rq_ssem,
    rq_rsem,
    ssem,
    rsem,
):
    dom = lax.axis_index("dom")
    grp = lax.axis_index("grp")
    n_dom = lax.axis_size("dom")
    chip = grp // 2
    core = grp % 2
    below = ((dom + n_dom - 1) % n_dom, grp)
    above = ((dom + 1) % n_dom, grp)

    def peer(i):
        dx, dc = PEERS[i]
        return ((chip + dx) % CHIPS) * 2 + (core + dc) % 2

    def origin(i):
        dx, dc = PEERS[i]
        return ((chip + CHIPS - dx) % CHIPS) * 2 + (core + dc) % 2

    targets = [(dom, peer(i)) for i in range(N_PEERS)] + [below, above]

    barrier = pltpu.get_barrier_semaphore()
    for target in targets:
        pl.semaphore_signal(barrier, inc=1, device_id=target, device_id_type=MESH)

    for f in range(4):
        partner = fpart[pl.ds(f, 1), :]
        for c in range(4):
            place = lax.broadcasted_iota(jnp.int32, (128, 128), 0) + 128 * c
            qm[pl.ds(128 * c, 128), pl.ds(128 * f, 128)] = jnp.where(place == partner, 1.0, 0.0)

    ids = cluster[...]
    idsf = ids.astype(F32)
    ids4 = jnp.broadcast_to(jnp.concatenate([idsf] * 4, axis=1), (8, 512))
    wanted = dot_nt(ids4, qm[128:512, :])
    for t in range(3):
        rq_send[t] = wanted[0:1, 128 * t : 128 * t + 128]

    pl.semaphore_wait(barrier, N_PEERS + 2)

    requests = []
    for i in range(N_PEERS):
        requests.append(
            pltpu.make_async_remote_copy(
                src_ref=rq_send.at[peer(i) // 8],
                dst_ref=rq_recv.at[grp],
                send_sem=rq_ssem.at[i],
                recv_sem=rq_rsem.at[i],
                device_id=targets[i],
                device_id_type=MESH,
            )
        )
    for j in range(2):
        requests.append(
            pltpu.make_async_remote_copy(
                src_ref=rq_send.at[2],
                dst_ref=rq_recv.at[N_GRP + j],
                send_sem=rq_ssem.at[N_PEERS + j],
                recv_sem=rq_rsem.at[N_PEERS + j],
                device_id=targets[N_PEERS + j],
                device_id_type=MESH,
            )
        )
    for copy in requests:
        copy.start()
    rq_recv[grp] = rq_send[grp // 8]

    rs[...] = jnp.zeros_like(rs)
    wpad[...] = jnp.zeros_like(wpad)
    for d in range(3):
        wpad[d, 0:56, 0:56] = stiff[d]
    for d in range(3):
        w = wpad[d]
        stack_weights(w[0:56], wk, pl.ds(56 * d, 56))
        stack_weights(jnp.transpose(w)[0:56], wown, pl.ds(56 * d, 56))

    for d in range(3):
        for p in range(QUANT):
            for q in range(QUANT):
                sb[(d * 9 + p) * 9 + q] = jnp.broadcast_to(jac[d, p, pl.ds(q, 1), :], (8, 128))

    for q in range(QUANT):
        x = old[q]
        store_operand(rs, q, 0, 56, x)
        for c in range(3):
            lev[c, q] = x * F32(TABLE[c][0])

    def step(k, carry):
        apply_modes(wk[...], rs, kx, 168)
        coef = []
        for c in range(3):
            value = F32(TABLE[c][5])
            for j in range(1, 5):
                value = jnp.where(k == j, F32(TABLE[c][j]), value)
            coef.append(value)
        for r0, rn in GROUPS:
            acc = [None] * QUANT
            for d in range(3):
                for p in range(QUANT):
                    x = kx[p, 56 * d + r0 : 56 * d + r0 + rn, :].reshape(rn // 8, 8, 128)
                    for q in range(QUANT):
                        term = x * sb[(d * 9 + p) * 9 + q][None]
                        acc[q] = term if acc[q] is None else acc[q] + term
            for q in range(QUANT):
                x = -acc[q].reshape(rn, 128)
                store_operand(rs, q, r0, rn, x)
                for c in range(3):
                    lev[c, q, pl.ds(r0, rn), :] = lev[c, q, pl.ds(r0, rn), :] + coef[c] * x
        return carry

    lax.fori_loop(1, ORDER, step, 0)

    for c in range(3):
        for q in range(QUANT):
            hi, lo = split(lev[c, q])
            lv[c, 56 * q : 56 * q + 56, 0:128] = hi
            lv[c, 56 * q : 56 * q + 56, 128:256] = lo
        lv[c, ROWS:WIRE, :] = jnp.zeros((WIRE - ROWS, 256), F32)

    for i in range(N_PEERS + 2):
        requests[i].wait_recv()
    asked = rq_recv[...].reshape(N_GRP + 2, 128)
    lane = lax.broadcasted_iota(jnp.int32, (128, 256), 1)
    sub = lax.broadcasted_iota(jnp.int32, (128, 256), 0)
    pick = jnp.where(sub == SHARE * (grp % 8) + lane % SHARE, 1.0, 0.0)
    spread = dot(asked[0:N_GRP], pick)
    rows = lax.broadcasted_iota(jnp.int32, (N_GRP, 256), 0)
    cols = lax.broadcasted_iota(jnp.int32, (N_GRP, 256), 1)
    peer_level = jnp.sum(jnp.where(rows == cols // SHARE, spread, 0.0), axis=0, keepdims=True)
    halo_lane = lax.broadcasted_iota(jnp.int32, (1, 128), 1)
    from_above = asked[N_GRP : N_GRP + 1]
    from_below = asked[N_GRP + 1 : N_GRP + 2]
    halo_level = jnp.where(
        halo_lane < HALO,
        pltpu.roll(jnp.broadcast_to(from_below, (8, 128)), 128 - HALO, 1)[0:1],
        pltpu.roll(jnp.broadcast_to(from_above, (8, 128)), HALO, 1)[0:1],
    )
    level_row = jnp.concatenate([peer_level, halo_level], axis=1)
    slot_row = jnp.concatenate([slots[...].astype(F32), jnp.zeros((1, 64), F32)], axis=1)
    code = level_row * 128.0 + slot_row
    code = jnp.transpose(jnp.broadcast_to(code, (128, 384)))[0:320]
    lane_f = lax.broadcasted_iota(jnp.int32, (320, 128), 1).astype(F32)
    total = None
    for c in range(3):
        a = jnp.where(code == lane_f + 128.0 * c, 1.0, 0.0)
        part = dot_nt(jnp.concatenate([a, a], axis=1), lv[c])
        total = part if total is None else total + part
    send[...] = total

    copies = []
    for i in range(N_PEERS):
        copies.append(
            pltpu.make_async_remote_copy(
                src_ref=send.at[pl.ds(pl.multiple_of(peer(i) * SHARE, SHARE), SHARE)],
                dst_ref=recv.at[pl.ds(pl.multiple_of(grp * SHARE, SHARE), SHARE)],
                send_sem=ssem.at[i],
                recv_sem=rsem.at[i],
                device_id=targets[i],
                device_id_type=MESH,
            )
        )
    for j in range(2):
        copies.append(
            pltpu.make_async_remote_copy(
                src_ref=send.at[pl.ds(GRP_SLOTS + HALO * j, HALO)],
                dst_ref=recv.at[pl.ds(GRP_SLOTS + HALO * (1 - j), HALO)],
                send_sem=ssem.at[N_PEERS + j],
                recv_sem=rsem.at[N_PEERS + j],
                device_id=targets[N_PEERS + j],
                device_id_type=MESH,
            )
        )
    for copy in copies:
        copy.start()
    mine = pl.ds(pl.multiple_of(grp * SHARE, SHARE), SHARE)
    recv[mine, :] = send[mine, :]

    for q in range(QUANT):
        x = jnp.where(ids == 0, lev[0, q], jnp.where(ids == 1, lev[1, q], lev[2, q]))
        store_operand(rs, q, 0, 56, x)
    for f in range(4):
        wpad[0, 0:56, 0:56] = lown[f]
        stack_weights(wpad[0, 0:56, :], wown, pl.ds(168 + 56 * f, 56))
    apply_modes(wown[...], rs, kx, 392)
    for r0, rn in GROUPS:
        acc = [old[q, pl.ds(r0, rn), :].reshape(rn // 8, 8, 128) for q in range(QUANT)]
        for d in range(3):
            for p in range(QUANT):
                x = kx[p, 56 * d + r0 : 56 * d + r0 + rn, :].reshape(rn // 8, 8, 128)
                for q in range(QUANT):
                    acc[q] = acc[q] + x * sb[(d * 9 + p) * 9 + q][None]
        for f in range(4):
            for p in range(QUANT):
                x = kx[p, 168 + 56 * f + r0 : 168 + 56 * f + r0 + rn, :].reshape(rn // 8, 8, 128)
                for q in range(QUANT):
                    s = jnp.broadcast_to(riem[0, f, p, pl.ds(q, 1), :], (8, 128))
                    acc[q] = acc[q] - x * s[None]
        for q in range(QUANT):
            upd[q, pl.ds(r0, rn), :] = acc[q].reshape(rn, 128)

    for half in range(2):
        sel = qm[0:128, 256 * half : 256 * half + 256]
        ids2 = jnp.concatenate([ids, ids], axis=1)
        total = None
        for c in range(3):
            m = jnp.where(ids2 == c, sel, 0.0)
            part = dot(lv[c], jnp.concatenate([m, m], axis=0))
            total = part if total is None else total + part
        near[2 * half] = total[:, 0:128]
        near[2 * half + 1] = total[:, 128:256]

    for f in range(4):
        for j in range(4):
            wpad[0, 0:56, 0:56] = lacross[f, j]
            stack_weights(wpad[0, 0:56, :], wx.at[f], pl.ds(56 * j, 56))

    def add_received(first, count, row0):
        block = jnp.transpose(recv[first : first + 128, :])
        hi, lo = split(block)
        lhs = jnp.concatenate([hi, lo], axis=1)
        for half in range(2):
            m = qm[row0 : row0 + 128, 256 * half : 256 * half + 256]
            part = dot(lhs, jnp.concatenate([m, m], axis=0))
            near[2 * half] = near[2 * half] + part[:, 0:128]
            near[2 * half + 1] = near[2 * half + 1] + part[:, 128:256]

    recv[320:384, :] = jnp.zeros((64, WIRE), F32)
    for j in range(2):
        copies[N_PEERS + j].wait_recv()
    add_received(256, 64, 384)
    for i in range(N_PEERS):
        copies[i].wait_recv()
    add_received(0, 128, 128)
    add_received(128, 128, 256)

    for f in range(4):
        for q in range(QUANT):
            store_operand(rs, q, 0, 56, near[f, 56 * q : 56 * q + 56, :])
        apply_modes(wx[f], rs, kx, 224)
        side = pface[pl.ds(f, 1), :]
        is0 = side == 0
        is1 = side == 1
        is2 = side == 2
        for r0, rn in GROUPS:
            acc = [upd[q, pl.ds(r0, rn), :].reshape(rn // 8, 8, 128) for q in range(QUANT)]
            for p in range(QUANT):
                parts = [kx[p, 56 * j + r0 : 56 * j + r0 + rn, :] for j in range(4)]
                x = jnp.where(is0, parts[0], jnp.where(is1, parts[1], jnp.where(is2, parts[2], parts[3])))
                x = x.reshape(rn // 8, 8, 128)
                for q in range(QUANT):
                    s = jnp.broadcast_to(riem[1, f, p, pl.ds(q, 1), :], (8, 128))
                    acc[q] = acc[q] - x * s[None]
            for q in range(QUANT):
                upd[q, pl.ds(r0, rn), :] = acc[q].reshape(rn, 128)

    first = [upd[q, 0:1, :] for q in range(6)]
    mean = (first[0] + first[1] + first[2]) / 3.0
    dev = [first[q] - mean if q < 3 else first[q] for q in range(6)]
    second = 0.5 * (dev[0] * dev[0] + dev[1] * dev[1] + dev[2] * dev[2])
    second = second + dev[3] * dev[3] + dev[4] * dev[4] + dev[5] * dev[5]
    strength = jnp.sqrt(second)
    limit = cohesion[...]
    excess = jnp.maximum(strength - limit, 0.0) / jnp.maximum(strength, limit)
    interval = jnp.where(ids == 0, base_step, jnp.where(ids == 1, 2.0 * base_step, 4.0 * base_step))
    factor = yflag[...].astype(F32) * excess * (1.0 - jnp.exp(-interval / relax_time[...]))
    pressure = (upd[0] + upd[1] + upd[2]) / 3.0
    for q in range(QUANT):
        x = upd[q]
        if q < 3:
            out[q] = x - factor * (x - pressure)
        elif q < 6:
            out[q] = x - factor * x
        else:
            out[q] = x

    for copy in requests:
        copy.wait_send()
    for copy in copies:
        copy.wait_send()


def on_device(
    old_state,
    stiffness,
    jacobians,
    lift_own,
    lift_across,
    riemann,
    cluster_ids,
    send_slots,
    face_partner,
    partner_face,
    cohesion,
    relax_time,
    yield_flag,
):
    vmem = pl.BlockSpec(memory_space=pltpu.VMEM)
    args = (
        old_state,
        stiffness,
        jacobians,
        lift_own,
        lift_across,
        riemann,
        cluster_ids.reshape(1, ELEM),
        send_slots.reshape(1, 320),
        face_partner,
        partner_face,
        cohesion.reshape(1, ELEM),
        relax_time.reshape(1, ELEM),
        yield_flag.reshape(1, ELEM),
    )
    return pl.pallas_call(
        kernel,
        out_shape=jax.ShapeDtypeStruct((QUANT, MODES, ELEM), F32),
        in_specs=[vmem] * len(args),
        out_specs=vmem,
        scratch_shapes=[
            pltpu.VMEM((256, 1152), F32),
            pltpu.VMEM((QUANT, 392, 128), F32),
            pltpu.VMEM((243, 8, 128), F32),
            pltpu.VMEM((3, 128, 128), F32),
            pltpu.VMEM((168, 256), F32),
            pltpu.VMEM((392, 256), F32),
            pltpu.VMEM((4, 224, 256), F32),
            pltpu.VMEM((512, 512), F32),
            pltpu.VMEM((3, QUANT, MODES, 128), F32),
            pltpu.VMEM((3, WIRE, 256), F32),
            pltpu.VMEM((4, WIRE, 128), F32),
            pltpu.VMEM((QUANT, MODES, 128), F32),
            pltpu.VMEM((320, WIRE), F32),
            pltpu.VMEM((384, WIRE), F32),
            pltpu.VMEM((3, 1, 128), F32),
            pltpu.VMEM((N_GRP + 2, 1, 128), F32),
            pltpu.SemaphoreType.DMA((N_PEERS + 2,)),
            pltpu.SemaphoreType.DMA((N_PEERS + 2,)),
            pltpu.SemaphoreType.DMA((N_PEERS + 2,)),
            pltpu.SemaphoreType.DMA((N_PEERS + 2,)),
        ],
        compiler_params=pltpu.CompilerParams(
            collective_id=0, has_side_effects=True, vmem_limit_bytes=48 * 1024 * 1024
        ),
    )(*args)


def solution(mesh):
    in_specs = (
        P(None, None, ("dom", "grp")),
        P(),
        P(None, None, None, ("dom", "grp")),
        P(),
        P(),
        P(None, None, None, None, ("dom", "grp")),
        P(("dom", "grp")),
        P(("dom", "grp")),
        P(None, ("dom", "grp")),
        P(None, ("dom", "grp")),
        P(("dom", "grp")),
        P(("dom", "grp")),
        P(("dom", "grp")),
    )
    out_specs = P(None, None, ("dom", "grp"))
    return jax.shard_map(
        on_device, mesh=mesh, in_specs=in_specs, out_specs=out_specs, check_vma=False
    )
```

```python
import jax
import jax.numpy as jnp
from jax import lax
from jax.experimental import pallas as pl
from jax.experimental.pallas import tpu as pltpu
from jax.sharding import PartitionSpec as P

QUANT = 9
MODES = 56
ORDER = 6
ELEM = 128
GRP_SLOTS = 256
HALO = 32
N_GRP = 16
SHARE = GRP_SLOTS // N_GRP
CHIPS = N_GRP // 2
ROWS = QUANT * MODES
WIRE = 512
MESH = pl.DeviceIdType.MESH
F32 = jnp.float32
base_step = 0.2

PEERS = ((4, 0), (4, 1), (3, 0), (3, 1), (-3, 0), (-3, 1), (0, 1), (0, 0)) + (
    (2, 0), (2, 1), (-2, 0), (-2, 1), (1, 0), (1, 1), (-1, 0), (-1, 1))
SELF = 7
OTHERS = tuple(i for i in range(N_GRP) if i != SELF)
RAW = 2
EARLY = RAW * SHARE
RAW_WIRE = 768
ASKED = tuple(i for i in OTHERS if i >= RAW)
QGROUPS = ((0, 4), (4, 8), (8, 9))


def taylor_table():
    entries = []
    for rate_level in range(3):
        interval = base_step * 2.0**rate_level
        factorial = 1.0
        powers = []
        for degree in range(ORDER):
            factorial = factorial * (degree + 1)
            powers.append(interval ** (degree + 1) / factorial)
        entries.append(powers)
    return entries


TABLE = taylor_table()


def split(x):
    hi = x.astype(jnp.bfloat16).astype(F32)
    return hi, x - hi


def dot(a, b):
    return lax.dot_general(a, b, (((1,), (0,)), ((), ())), preferred_element_type=F32)


def dot_nt(a, b):
    return lax.dot_general(a, b, (((1,), (1,)), ((), ())), preferred_element_type=F32)


def stack_weights(w, dst, rows):
    hi, lo = split(w)
    dst[rows, 0:128] = hi + pltpu.roll(hi, 64, 1)
    dst[rows, 128:256] = lo


def store_operand(rs, q, x):
    hi, lo = split(x)
    lanes = pl.ds(q * 128, 128)
    rs[0:56, lanes] = hi
    rs[64:120, lanes] = lo
    rs[128:184, lanes] = hi


def apply_modes(w, rs, kx, rows, j):
    if j < 4:
        out = dot(w, rs[:, 256 * j : 256 * j + 256])
        kx[2 * j, 0:rows, :] = out[:, 0:128]
        kx[2 * j + 1, 0:rows, :] = out[:, 128:256]
    else:
        kx[8, 0:rows, :] = dot(w, rs[:, 1024:1152])


def tiles(x):
    return x.reshape(7, 8, 128)


def kernel(
    old_h,
    stiff_h,
    jac_h,
    lown_h,
    lacross_h,
    riem_h,
    cluster_h,
    slots_h,
    fpart_h,
    pface_h,
    cohesion_h,
    relax_h,
    yflag_h,
    out,
    old,
    stiff,
    jac,
    lown,
    lacross,
    riem,
    cluster,
    slots,
    fpart,
    pface,
    cohesion,
    relax_time,
    yflag,
    rs,
    kx,
    sb,
    wpad,
    wk,
    wown,
    wx,
    qm,
    lev,
    lv,
    sel,
    picked,
    near,
    chosen,
    upd,
    send,
    recv,
    raw,
    raw_send,
    raw_recv,
    raw_state,
    raw_sb,
    raw_near,
    rq_send,
    rq_recv,
    load_sem,
    rq_ssem,
    rq_rsem,
    ssem,
    rsem,
    met_sem,
):
    dom = lax.axis_index("dom")
    grp = lax.axis_index("grp")
    n_dom = lax.axis_size("dom")
    chip = grp // 2
    core = grp % 2
    below = ((dom + n_dom - 1) % n_dom, grp)
    above = ((dom + 1) % n_dom, grp)

    def peer(i):
        dx, dc = PEERS[i]
        return ((chip + dx + CHIPS) % CHIPS) * 2 + (core + dc) % 2

    def origin(i):
        dx, dc = PEERS[i]
        return ((chip - dx + CHIPS) % CHIPS) * 2 + (core + dc) % 2

    barrier = pltpu.get_barrier_semaphore()
    partner_core = (dom, chip * 2 + 1 - core)
    for i in OTHERS:
        if PEERS[i][1] == 0:

            @pl.when(core == 0)
            def _(i=i):
                pl.semaphore_signal(barrier, inc=1, device_id=(dom, peer(i)), device_id_type=MESH)

        else:

            @pl.when(core == 1)
            def _(i=i):
                pl.semaphore_signal(barrier, inc=1, device_id=(dom, peer(i)), device_id_type=MESH)

    for target in (below, above):
        pl.semaphore_signal(barrier, inc=1, device_id=(target[0], chip * 2 + 1), device_id_type=MESH)

    names = ("fpart", "cluster", "stiff", "old", "jac", "slots", "lown", "lacross", "riem", "pface", "coh", "relax", "flag")
    pairs = (
        (fpart_h, fpart), (cluster_h, cluster), (stiff_h, stiff), (old_h, old), (jac_h, jac), (slots_h, slots),
        (lown_h, lown), (lacross_h, lacross), (riem_h, riem), (pface_h, pface), (cohesion_h, cohesion),
        (relax_h, relax_time), (yflag_h, yflag),
    )
    loads = {}
    for n, (name, (src, dst)) in enumerate(zip(names, pairs)):
        loads[name] = pltpu.make_async_copy(src, dst, load_sem.at[n])
        loads[name].start()

    rs[...] = jnp.zeros_like(rs)
    wpad[...] = jnp.zeros_like(wpad)

    loads["fpart"].wait()
    loads["cluster"].wait()
    iota128 = lax.broadcasted_iota(jnp.int32, (128, 128), 0)
    iota16 = lax.broadcasted_iota(jnp.int32, (SHARE, 128), 0)
    for f in range(4):
        partner = fpart[pl.ds(f, 1), :]
        lanes = pl.ds(128 * f, 128)
        qm[0:128, lanes] = jnp.where(iota128 == partner, 1.0, 0.0)
        for i in range(N_GRP):
            moved = partner - (ELEM + SHARE * origin(i))
            qm[pl.ds(ELEM + SHARE * i, SHARE), lanes] = jnp.where(iota16 == moved, 1.0, 0.0)
        qm[384:512, lanes] = jnp.where(iota128 + 384 == partner, 1.0, 0.0)

    ids = cluster[...]
    idsf = ids.astype(F32)
    ids4 = jnp.broadcast_to(jnp.concatenate([idsf] * 4, axis=1), (8, 512))
    wanted = dot_nt(ids4, qm[128:512, :])
    for t in range(3):
        rq_send[t] = wanted[0:1, 128 * t : 128 * t + 128]
    rq_recv[SELF] = wanted[0:1, 0:128]
    for i in range(RAW):
        rq_recv[i] = jnp.zeros((1, 128), F32)

    loads["stiff"].wait()
    for d in range(3):
        wpad[d, 0:56, 0:56] = stiff[d]
    for d in range(3):
        w = wpad[d]
        stack_weights(-w[0:56], wk, pl.ds(56 * d, 56))
        stack_weights(jnp.transpose(w)[0:56], wown, pl.ds(56 * d, 56))
    loads["old"].wait()
    for q in range(QUANT):
        x = old[q]
        store_operand(rs.at[0], q, x)
        for c in range(3):
            lev[c, q] = x * F32(TABLE[c][0])
    loads["jac"].wait()
    for p in range(QUANT):
        for q in range(QUANT):
            for d in range(3):
                sb[(p * 9 + q) * 3 + d] = jnp.broadcast_to(jac[p, q, pl.ds(d, 1), :], (8, 128))

    for j in range(5):
        apply_modes(wk[...], rs.at[0], kx.at[0], 168, j)

    loads["slots"].wait()
    lane = lax.broadcasted_iota(jnp.int32, (1, 256), 1)
    place = lane % SHARE
    for i in range(N_GRP):
        place = place + jnp.where(lane // SHARE == i, SHARE * peer(i), 0)
    order = jnp.where(lax.broadcasted_iota(jnp.int32, (256, 256), 0) == place, 1.0, 0.0)
    slot_row = slots[...].astype(F32).reshape(1, 320)
    moved = dot(jnp.broadcast_to(slot_row[:, 0:256], (8, 256)), order)[0:1]
    slot_row = jnp.concatenate([moved, slot_row[:, 256:320], jnp.zeros((1, 64), F32)], axis=1)
    slot_col = jnp.transpose(jnp.broadcast_to(slot_row, (128, 384)))[0:320]
    lane_f = lax.broadcasted_iota(jnp.int32, (320, 128), 1).astype(F32)
    onehot = jnp.where(slot_col == lane_f, 1.0, 0.0)
    sel[:, 0:128] = onehot
    sel[:, 128:256] = onehot

    for q in range(QUANT):
        hi, lo = split(old[q])
        raw[56 * q : 56 * q + 56, 0:128] = hi
        raw[56 * q : 56 * q + 56, 128:256] = lo
    raw[ROWS:WIRE, :] = jnp.zeros((WIRE - ROWS, 256), F32)
    sub8 = lax.broadcasted_iota(jnp.int32, (8, 128), 0)
    for t in range(32):
        x = jnp.zeros((8, 128), F32)
        for i in range(8):
            if 8 * t + i < 243:
                x = jnp.where(sub8 == i, sb[8 * t + i], x)
        hi, lo = split(x)
        raw[WIRE + 8 * t : WIRE + 8 * t + 8, 0:128] = hi
        raw[WIRE + 8 * t : WIRE + 8 * t + 8, 128:256] = lo
    for n in range(3):
        raw_send[:, 256 * n : 256 * n + 256] = dot_nt(sel[0:EARLY, :], raw[256 * n : 256 * n + 256, :])
    raw_recv[EARLY:128, :] = jnp.zeros((128 - EARLY, RAW_WIRE), F32)

    def taylor_step(k, table, flip, take):
        src, dst = kx.at[(k - 1 + flip) % 2], kx.at[(k + flip) % 2]
        made = rs.at[(k + flip) % 2]
        for q0, q1 in QGROUPS:
            acc = {}
            for p in range(QUANT):
                for d in range(3):
                    x = tiles(src[p, 56 * d : 56 * d + 56, :])
                    for q in range(q0, q1):
                        term = x * table[(p * 9 + q) * 3 + d][None]
                        acc[q] = term if q not in acc else acc[q] + term
            for q in range(q0, q1):
                x = acc[q].reshape(56, 128)
                if k < ORDER - 1:
                    store_operand(made, q, x)
                take(k, q, x)
            if k < ORDER - 1:
                for j in range(q0 // 2, (q1 + 1) // 2):
                    apply_modes(wk[...], made, dst, 168, j)

    def take_levels(k, q, x):
        for c in range(3):
            total = lev[c, q] + F32(TABLE[c][k]) * x
            lev[c, q] = total
            if k == ORDER - 1:
                hi, lo = split(total)
                lv[c, 56 * q : 56 * q + 56, 0:128] = hi
                lv[c, 56 * q : 56 * q + 56, 128:256] = lo

    taylor_step(1, sb, 0, take_levels)

    @pl.when(core == 0)
    def _():
        pl.semaphore_wait(barrier, len(OTHERS))
        pl.semaphore_signal(met_sem.at[0], inc=1, device_id=partner_core, device_id_type=MESH)

    @pl.when(core == 1)
    def _():
        pl.semaphore_wait(met_sem.at[0], 1)

    requests = []
    for i in ASKED:
        requests.append(
            pltpu.make_async_remote_copy(
                src_ref=rq_send.at[i // 8],
                dst_ref=rq_recv.at[i],
                send_sem=rq_ssem.at[i],
                recv_sem=rq_rsem.at[i],
                device_id=(dom, origin(i)),
                device_id_type=MESH,
            )
        )
    for copy in requests:
        copy.start()
    copies = {}
    for i in range(RAW):
        copies[i] = pltpu.make_async_remote_copy(
            src_ref=raw_send.at[pl.ds(SHARE * i, SHARE)],
            dst_ref=raw_recv.at[pl.ds(SHARE * i, SHARE)],
            send_sem=ssem.at[i],
            recv_sem=rsem.at[i],
            device_id=(dom, peer(i)),
            device_id_type=MESH,
        )
        copies[i].start()
    loads["lown"].wait()

    for k in range(2, ORDER):
        taylor_step(k, sb, 0, take_levels)
    for c in range(3):
        lv[c, ROWS:WIRE, :] = jnp.zeros((WIRE - ROWS, 256), F32)
    for h in range(2):
        for c in range(3):
            picked[c, EARLY:320, 256 * h : 256 * h + 256] = dot_nt(
                sel[EARLY:320, :], lv[c, 256 * h : 256 * h + 256, :]
            )

    for copy in requests:
        copy.wait_recv()
    asked = rq_recv[0:N_GRP].reshape(N_GRP, 128)
    block = lax.broadcasted_iota(jnp.int32, (8, 128), 0)
    lane8 = lax.broadcasted_iota(jnp.int32, (8, 128), 1)
    rows = []
    for t in range(2):
        mine = jnp.where(block == lane8 // SHARE, asked[8 * t : 8 * t + 8], 0.0)
        rows.append(jnp.sum(mine, axis=0, keepdims=True))
    def fill(t, row, start, stop):
        span = pl.ds(128 * t + start, stop - start)
        col = jnp.transpose(jnp.broadcast_to(row, (128, 128)))[start:stop]
        is0 = col < 0.5
        is1 = col < 1.5
        for n in range(4):
            lanes = pl.ds(128 * n, 128)
            send[span, lanes] = jnp.where(
                is0, picked[0, span, lanes], jnp.where(is1, picked[1, span, lanes], picked[2, span, lanes])
            )

    fill(0, rows[0], EARLY, 128)
    fill(1, rows[1], 0, 128)

    for i in ASKED:
        copies[i] = pltpu.make_async_remote_copy(
            src_ref=send.at[pl.ds(SHARE * i, SHARE)],
            dst_ref=recv.at[pl.ds(SHARE * i, SHARE)],
            send_sem=ssem.at[i],
            recv_sem=rsem.at[i],
            device_id=(dom, peer(i)),
            device_id_type=MESH,
        )
    for i in copies:
        if i >= RAW:
            copies[i].start()
    recv[SHARE * SELF : SHARE * SELF + SHARE, :] = send[SHARE * SELF : SHARE * SELF + SHARE, :]

    for name in ("lacross", "riem", "pface", "coh", "relax"):
        loads[name].wait()

    @pl.when(core == 1)
    def _():
        pl.semaphore_wait(barrier, 4)
        pl.semaphore_signal(met_sem.at[1], inc=1, device_id=partner_core, device_id_type=MESH)

    @pl.when(core == 0)
    def _():
        pl.semaphore_wait(met_sem.at[1], 1)

    halo_requests = []
    for j, target in enumerate((below, above)):
        halo_requests.append(
            pltpu.make_async_remote_copy(
                src_ref=rq_send.at[2],
                dst_ref=rq_recv.at[N_GRP + j],
                send_sem=rq_ssem.at[N_GRP + j],
                recv_sem=rq_rsem.at[N_GRP + j],
                device_id=target,
                device_id_type=MESH,
            )
        )
    for copy in halo_requests:
        copy.start()
    loads["flag"].wait()

    for q in range(QUANT):
        x = jnp.where(ids == 0, lev[0, q], jnp.where(ids == 1, lev[1, q], lev[2, q]))
        store_operand(rs.at[0], q, x)
    for f in range(4):
        wpad[0, 0:56, 0:56] = lown[f]
        stack_weights(wpad[0, 0:56, :], wown, pl.ds(168 + 56 * f, 56))
    for j in range(5):
        apply_modes(wown[...], rs.at[0], kx.at[0], 392, j)

    def trace_terms(source, row0, side, f, acc, q0, q1):
        for p in range(QUANT):
            x = tiles(source[p, row0 : row0 + 56, :])
            for q in range(q0, q1):
                s = jnp.broadcast_to(riem[side, p, q, pl.ds(f, 1), :], (8, 128))
                acc[q] = acc[q] - x * s[None]

    for q0, q1 in QGROUPS:
        acc = {q: tiles(old[q]) for q in range(q0, q1)}
        for p in range(QUANT):
            for d in range(3):
                x = tiles(kx[0, p, 56 * d : 56 * d + 56, :])
                for q in range(q0, q1):
                    acc[q] = acc[q] + x * sb[(p * 9 + q) * 3 + d][None]
        for f in range(4):
            trace_terms(kx.at[0], 168 + 56 * f, 0, f, acc, q0, q1)
        for q in range(q0, q1):
            upd[q] = acc[q].reshape(56, 128)

    for copy in halo_requests:
        copy.wait_recv()
    from_above = jnp.broadcast_to(rq_recv[N_GRP], (8, 128))
    from_below = jnp.broadcast_to(rq_recv[N_GRP + 1], (8, 128))
    halo = jnp.where(
        lane8 < HALO, pltpu.roll(from_below, 128 - HALO, 1), pltpu.roll(from_above, HALO, 1)
    )
    fill(2, halo[0:1], 0, 64)
    for j, target in enumerate((below, above)):
        copies[N_GRP + j] = pltpu.make_async_remote_copy(
            src_ref=send.at[pl.ds(GRP_SLOTS + HALO * j, HALO)],
            dst_ref=recv.at[pl.ds(GRP_SLOTS + HALO * (1 - j), HALO)],
            send_sem=ssem.at[N_GRP + j],
            recv_sem=rsem.at[N_GRP + j],
            device_id=target,
            device_id_type=MESH,
        )
    for j in range(2):
        copies[N_GRP + j].start()
    for i in range(RAW):
        copies[i].wait_recv()

    ids2 = jnp.concatenate([ids, ids], axis=1)
    for half in range(2):
        m = qm[0:128, 256 * half : 256 * half + 256]
        total = None
        for c in range(3):
            mc = jnp.where(ids2 == c, m, 0.0)
            part = dot(lv[c], jnp.concatenate([mc, mc], axis=0))
            total = part if total is None else total + part
        near[2 * half] = total[:, 0:128]
        near[2 * half + 1] = total[:, 128:256]

    for f in range(4):
        for j in range(4):
            wpad[0, 0:56, 0:56] = lacross[f, j]
            stack_weights(wpad[0, 0:56, :], wx.at[f], pl.ds(56 * j, 56))

    raw_state[...] = jnp.transpose(raw_recv[...])
    for r in range(243):
        raw_sb[r] = jnp.broadcast_to(raw_state[pl.ds(WIRE + r, 1), :], (8, 128))
    level = rq_send[0]

    def weight(k):
        return jnp.where(level < 0.5, TABLE[0][k], jnp.where(level < 1.5, TABLE[1][k], TABLE[2][k]))

    def take_near(k, q, x):
        raw_near[56 * q : 56 * q + 56, :] = raw_near[56 * q : 56 * q + 56, :] + weight(k) * x

    for q in range(QUANT):
        x = raw_state[56 * q : 56 * q + 56, :]
        store_operand(rs.at[1], q, x)
        raw_near[56 * q : 56 * q + 56, :] = weight(0) * x
    raw_near[ROWS:WIRE, :] = jnp.zeros((WIRE - ROWS, 128), F32)
    for j in range(5):
        apply_modes(wk[...], rs.at[1], kx.at[1], 168, j)
    for k in range(1, ORDER):
        taylor_step(k, raw_sb, 1, take_near)

    def add_received(first, row0, extra):
        block = jnp.transpose(recv[first : first + 128, :])
        if extra is not None:
            block = block + extra
        hi, lo = split(block)
        lhs = jnp.concatenate([hi, lo], axis=1)
        for half in range(2):
            m = qm[row0 : row0 + 128, 256 * half : 256 * half + 256]
            part = dot(lhs, jnp.concatenate([m, m], axis=0))
            near[2 * half] = near[2 * half] + part[:, 0:128]
            near[2 * half + 1] = near[2 * half + 1] + part[:, 128:256]

    recv[320:384, :] = jnp.zeros((64, WIRE), F32)
    recv[0:EARLY, :] = jnp.zeros((EARLY, WIRE), F32)
    for j in range(2):
        copies[N_GRP + j].wait_recv()
    add_received(256, 384, None)
    for i in range(RAW, 8):
        if i != SELF:
            copies[i].wait_recv()
    add_received(0, 128, raw_near[...])
    for i in range(8, 16):
        copies[i].wait_recv()
    add_received(128, 256, None)

    for f in range(4):
        work = rs.at[f % 2]
        lifted = kx.at[f % 2]
        side = pface[pl.ds(f, 1), :]
        is0 = side == 0
        is1 = side == 1
        is2 = side == 2
        for q in range(QUANT):
            store_operand(work, q, near[f, 56 * q : 56 * q + 56, :])
        for j in range(5):
            apply_modes(wx[f], work, lifted, 224, j)
        for p in range(QUANT):
            parts = [lifted[p, 56 * j : 56 * j + 56, :] for j in range(4)]
            chosen[f % 2, p] = jnp.where(
                is0, parts[0], jnp.where(is1, parts[1], jnp.where(is2, parts[2], parts[3]))
            )
        for q0, q1 in QGROUPS:
            acc = {q: tiles(upd[q]) for q in range(q0, q1)}
            trace_terms(chosen.at[f % 2], 0, 1, f, acc, q0, q1)
            for q in range(q0, q1):
                upd[q] = acc[q].reshape(56, 128)

    first = [upd[q, 0:1, :] for q in range(6)]
    mean = (first[0] + first[1] + first[2]) / 3.0
    dev = [first[q] - mean if q < 3 else first[q] for q in range(6)]
    second = 0.5 * (dev[0] * dev[0] + dev[1] * dev[1] + dev[2] * dev[2])
    second = second + dev[3] * dev[3] + dev[4] * dev[4] + dev[5] * dev[5]
    strength = jnp.sqrt(second)
    limit = cohesion[...]
    excess = jnp.maximum(strength - limit, 0.0) / jnp.maximum(strength, limit)
    interval = jnp.where(ids == 0, base_step, jnp.where(ids == 1, 2.0 * base_step, 4.0 * base_step))
    factor = yflag[...].astype(F32) * excess * (1.0 - jnp.exp(-interval / relax_time[...]))
    pressure = (upd[0] + upd[1] + upd[2]) * F32(1.0 / 3.0)
    for q in range(QUANT):
        x = upd[q]
        if q < 3:
            out[q] = x - factor * (x - pressure)
        elif q < 6:
            out[q] = x - factor * x
        else:
            out[q] = x

    for copy in requests + halo_requests:
        copy.wait_send()
    for copy in copies.values():
        copy.wait_send()


def on_device(
    old_state,
    stiffness,
    jacobians,
    lift_own,
    lift_across,
    riemann,
    cluster_ids,
    send_slots,
    face_partner,
    partner_face,
    cohesion,
    relax_time,
    yield_flag,
):
    args = (
        old_state,
        stiffness,
        jnp.transpose(jacobians, (1, 2, 0, 3)),
        lift_own,
        lift_across,
        jnp.transpose(riemann, (0, 2, 3, 1, 4)),
        cluster_ids.reshape(1, ELEM),
        send_slots,
        face_partner,
        partner_face,
        cohesion.reshape(1, ELEM),
        relax_time.reshape(1, ELEM),
        yield_flag.reshape(1, ELEM),
    )
    args = tuple(pltpu.with_memory_space_constraint(a, pltpu.HBM) for a in args)
    sems = [pltpu.SemaphoreType.DMA((N_GRP + 2,)) for _ in range(4)]
    return pl.pallas_call(
        kernel,
        out_shape=jax.ShapeDtypeStruct((QUANT, MODES, ELEM), F32),
        in_specs=[pl.BlockSpec(memory_space=pltpu.HBM)] * len(args),
        out_specs=pl.BlockSpec(memory_space=pltpu.VMEM),
        scratch_shapes=[pltpu.VMEM(a.shape, a.dtype) for a in args]
        + [
            pltpu.VMEM((2, 256, 1152), F32),
            pltpu.VMEM((2, QUANT, 392, 128), F32),
            pltpu.VMEM((243, 8, 128), F32),
            pltpu.VMEM((3, 128, 128), F32),
            pltpu.VMEM((168, 256), F32),
            pltpu.VMEM((392, 256), F32),
            pltpu.VMEM((4, 224, 256), F32),
            pltpu.VMEM((512, 512), F32),
            pltpu.VMEM((3, QUANT, MODES, 128), F32),
            pltpu.VMEM((3, WIRE, 256), F32),
            pltpu.VMEM((320, 256), F32),
            pltpu.VMEM((3, 320, WIRE), F32),
            pltpu.VMEM((4, WIRE, 128), F32),
            pltpu.VMEM((2, QUANT, MODES, 128), F32),
            pltpu.VMEM((QUANT, MODES, 128), F32),
            pltpu.VMEM((320, WIRE), F32),
            pltpu.VMEM((384, WIRE), F32),
            pltpu.VMEM((RAW_WIRE, 256), F32),
            pltpu.VMEM((EARLY, RAW_WIRE), F32),
            pltpu.VMEM((128, RAW_WIRE), F32),
            pltpu.VMEM((RAW_WIRE, 128), F32),
            pltpu.VMEM((243, 8, 128), F32),
            pltpu.VMEM((WIRE, 128), F32),
            pltpu.VMEM((3, 1, 128), F32),
            pltpu.VMEM((N_GRP + 2, 1, 128), F32),
            pltpu.SemaphoreType.DMA((13,)),
        ]
        + sems
        + [pltpu.SemaphoreType.REGULAR((2,))],
        compiler_params=pltpu.CompilerParams(
            collective_id=0, has_side_effects=True, vmem_limit_bytes=40 * 1024 * 1024
        ),
    )(*args)


def solution(mesh):
    in_specs = (
        P(None, None, ("dom", "grp")),
        P(),
        P(None, None, None, ("dom", "grp")),
        P(),
        P(),
        P(None, None, None, None, ("dom", "grp")),
        P(("dom", "grp")),
        P(("dom", "grp")),
        P(None, ("dom", "grp")),
        P(None, ("dom", "grp")),
        P(("dom", "grp")),
        P(("dom", "grp")),
        P(("dom", "grp")),
    )
    out_specs = P(None, None, ("dom", "grp"))
    return jax.shard_map(
        on_device, mesh=mesh, in_specs=in_specs, out_specs=out_specs, check_vma=False
    )
```

```python
import jax
import jax.numpy as jnp
from jax import lax
from jax.experimental import pallas as pl
from jax.experimental.pallas import tpu as pltpu
from jax.sharding import PartitionSpec as P

QUANT = 9
MODES = 56
ORDER = 6
ELEM = 128
GRP_SLOTS = 256
HALO = 32
N_GRP = 16
SHARE = GRP_SLOTS // N_GRP
CHIPS = N_GRP // 2
ROWS = QUANT * MODES
WIRE = 512
MESH = pl.DeviceIdType.MESH
F32 = jnp.float32
base_step = 0.2

PEERS = ((4, 0), (4, 1), (3, 0), (3, 1), (-3, 0), (-3, 1), (0, 1), (0, 0)) + (
    (2, 0), (2, 1), (-2, 0), (-2, 1), (1, 0), (1, 1), (-1, 0), (-1, 1))
SELF = 7
OTHERS = tuple(i for i in range(N_GRP) if i != SELF)
RAW = 2
EARLY = RAW * SHARE
RAW_WIRE = 768
ASKED = tuple(i for i in OTHERS if i >= RAW)
QGROUPS = ((0, 4), (4, 8), (8, 9))


def taylor_table():
    entries = []
    for rate_level in range(3):
        interval = base_step * 2.0**rate_level
        factorial = 1.0
        powers = []
        for degree in range(ORDER):
            factorial = factorial * (degree + 1)
            powers.append(interval ** (degree + 1) / factorial)
        entries.append(powers)
    return entries


TABLE = taylor_table()


def split(x):
    hi = x.astype(jnp.bfloat16).astype(F32)
    return hi, x - hi


def dot(a, b):
    return lax.dot_general(a, b, (((1,), (0,)), ((), ())), preferred_element_type=F32)


def dot_nt(a, b):
    return lax.dot_general(a, b, (((1,), (1,)), ((), ())), preferred_element_type=F32)


def stack_weights(w, dst, rows):
    hi, lo = split(w)
    dst[rows, 0:128] = hi + pltpu.roll(hi, 64, 1)
    dst[rows, 128:256] = lo


def store_operand(rs, q, x):
    hi, lo = split(x)
    lanes = pl.ds(q * 128, 128)
    rs[0:56, lanes] = hi
    rs[64:120, lanes] = lo
    rs[128:184, lanes] = hi


def apply_modes(w, rs, kx, rows, j):
    if j < 4:
        out = dot(w, rs[:, 256 * j : 256 * j + 256])
        kx[2 * j, 0:rows, :] = out[:, 0:128]
        kx[2 * j + 1, 0:rows, :] = out[:, 128:256]
    else:
        kx[8, 0:rows, :] = dot(w, rs[:, 1024:1152])


def tiles(x):
    return x.reshape(7, 8, 128)


def kernel(
    old_h,
    stiff_h,
    jac_h,
    lown_h,
    lacross_h,
    riem_h,
    cluster_h,
    slots_h,
    fpart_h,
    pface_h,
    cohesion_h,
    relax_h,
    yflag_h,
    out,
    old,
    stiff,
    jac,
    lown,
    lacross,
    riem,
    cluster,
    slots,
    fpart,
    pface,
    cohesion,
    relax_time,
    yflag,
    rs,
    kx,
    sb,
    wpad,
    wk,
    wown,
    wx,
    qm,
    lev,
    lv,
    sel,
    picked,
    near,
    chosen,
    upd,
    send,
    recv,
    raw,
    raw_send,
    raw_recv,
    raw_state,
    raw_sb,
    raw_near,
    rq_send,
    rq_recv,
    load_sem,
    rq_ssem,
    rq_rsem,
    ssem,
    rsem,
    met_sem,
):
    dom = lax.axis_index("dom")
    grp = lax.axis_index("grp")
    n_dom = lax.axis_size("dom")
    chip = grp // 2
    core = grp % 2
    below = ((dom + n_dom - 1) % n_dom, grp)
    above = ((dom + 1) % n_dom, grp)

    def peer(i):
        dx, dc = PEERS[i]
        return ((chip + dx + CHIPS) % CHIPS) * 2 + (core + dc) % 2

    def origin(i):
        dx, dc = PEERS[i]
        return ((chip - dx + CHIPS) % CHIPS) * 2 + (core + dc) % 2

    barrier = pltpu.get_barrier_semaphore()
    partner_core = (dom, chip * 2 + 1 - core)
    for i in OTHERS:
        if PEERS[i][1] == 0:

            @pl.when(core == 0)
            def _(i=i):
                pl.semaphore_signal(barrier, inc=1, device_id=(dom, peer(i)), device_id_type=MESH)

        else:

            @pl.when(core == 1)
            def _(i=i):
                pl.semaphore_signal(barrier, inc=1, device_id=(dom, peer(i)), device_id_type=MESH)

    for target in (below, above):
        pl.semaphore_signal(barrier, inc=1, device_id=(target[0], chip * 2 + 1), device_id_type=MESH)

    names = ("fpart", "cluster", "stiff", "old", "jac", "slots", "lown", "lacross", "riem", "pface", "coh", "relax", "flag")
    pairs = (
        (fpart_h, fpart), (cluster_h, cluster), (stiff_h, stiff), (old_h, old), (jac_h, jac), (slots_h, slots),
        (lown_h, lown), (lacross_h, lacross), (riem_h, riem), (pface_h, pface), (cohesion_h, cohesion),
        (relax_h, relax_time), (yflag_h, yflag),
    )
    loads = {}
    for n, (name, (src, dst)) in enumerate(zip(names, pairs)):
        loads[name] = pltpu.make_async_copy(src, dst, load_sem.at[n])
        loads[name].start()

    rs[...] = jnp.zeros_like(rs)
    wpad[...] = jnp.zeros_like(wpad)

    loads["fpart"].wait()
    loads["cluster"].wait()
    iota128 = lax.broadcasted_iota(jnp.int32, (128, 128), 0)
    iota16 = lax.broadcasted_iota(jnp.int32, (SHARE, 128), 0)
    for f in range(4):
        partner = fpart[pl.ds(f, 1), :]
        lanes = pl.ds(128 * f, 128)
        qm[0:128, lanes] = jnp.where(iota128 == partner, 1.0, 0.0)
        for i in range(N_GRP):
            moved = partner - (ELEM + SHARE * origin(i))
            qm[pl.ds(ELEM + SHARE * i, SHARE), lanes] = jnp.where(iota16 == moved, 1.0, 0.0)
        qm[384:512, lanes] = jnp.where(iota128 + 384 == partner, 1.0, 0.0)

    ids = cluster[...]
    idsf = ids.astype(F32)
    ids4 = jnp.broadcast_to(jnp.concatenate([idsf] * 4, axis=1), (8, 512))
    wanted = dot_nt(ids4, qm[128:512, :])
    for t in range(3):
        rq_send[t] = wanted[0:1, 128 * t : 128 * t + 128]
    rq_recv[SELF] = wanted[0:1, 0:128]
    for i in range(RAW):
        rq_recv[i] = jnp.zeros((1, 128), F32)

    loads["stiff"].wait()
    for d in range(3):
        wpad[d, 0:56, 0:56] = stiff[d]
    for d in range(3):
        w = wpad[d]
        stack_weights(-w[0:56], wk, pl.ds(56 * d, 56))
        stack_weights(jnp.transpose(w)[0:56], wown, pl.ds(56 * d, 56))
    loads["old"].wait()
    for q in range(QUANT):
        x = old[q]
        store_operand(rs.at[0], q, x)
        for c in range(3):
            lev[c, q] = x * F32(TABLE[c][0])
    loads["jac"].wait()
    for p in range(QUANT):
        for q in range(QUANT):
            for d in range(3):
                sb[(p * 9 + q) * 3 + d] = jnp.broadcast_to(jac[p, q, pl.ds(d, 1), :], (8, 128))

    for j in range(5):
        apply_modes(wk[...], rs.at[0], kx.at[0], 168, j)

    loads["slots"].wait()
    lane = lax.broadcasted_iota(jnp.int32, (1, 256), 1)
    place = lane % SHARE
    for i in range(N_GRP):
        place = place + jnp.where(lane // SHARE == i, SHARE * peer(i), 0)
    order = jnp.where(lax.broadcasted_iota(jnp.int32, (256, 256), 0) == place, 1.0, 0.0)
    slot_row = slots[...].astype(F32).reshape(1, 320)
    moved = dot(jnp.broadcast_to(slot_row[:, 0:256], (8, 256)), order)[0:1]
    slot_row = jnp.concatenate([moved, slot_row[:, 256:320], jnp.zeros((1, 64), F32)], axis=1)
    slot_col = jnp.transpose(jnp.broadcast_to(slot_row, (128, 384)))[0:320]
    lane_f = lax.broadcasted_iota(jnp.int32, (320, 128), 1).astype(F32)
    onehot = jnp.where(slot_col == lane_f, 1.0, 0.0)
    sel[:, 0:128] = onehot
    sel[:, 128:256] = onehot

    for q in range(QUANT):
        hi, lo = split(old[q])
        raw[56 * q : 56 * q + 56, 0:128] = hi
        raw[56 * q : 56 * q + 56, 128:256] = lo
    raw[ROWS:WIRE, :] = jnp.zeros((WIRE - ROWS, 256), F32)
    sub8 = lax.broadcasted_iota(jnp.int32, (8, 128), 0)
    for t in range(32):
        x = jnp.zeros((8, 128), F32)
        for i in range(8):
            if 8 * t + i < 243:
                x = jnp.where(sub8 == i, sb[8 * t + i], x)
        hi, lo = split(x)
        raw[WIRE + 8 * t : WIRE + 8 * t + 8, 0:128] = hi
        raw[WIRE + 8 * t : WIRE + 8 * t + 8, 128:256] = lo
    for n in range(3):
        raw_send[:, 256 * n : 256 * n + 256] = dot_nt(sel[0:EARLY, :], raw[256 * n : 256 * n + 256, :])
    raw_recv[EARLY:128, :] = jnp.zeros((128 - EARLY, RAW_WIRE), F32)

    def taylor_step(k, table, flip, take):
        src, dst = kx.at[(k - 1 + flip) % 2], kx.at[(k + flip) % 2]
        made = rs.at[(k + flip) % 2]
        for q0, q1 in QGROUPS:
            acc = {}
            for p in range(QUANT):
                for d in range(3):
                    x = tiles(src[p, 56 * d : 56 * d + 56, :])
                    for q in range(q0, q1):
                        term = x * table[(p * 9 + q) * 3 + d][None]
                        acc[q] = term if q not in acc else acc[q] + term
            for q in range(q0, q1):
                x = acc[q].reshape(56, 128)
                if k < ORDER - 1:
                    store_operand(made, q, x)
                take(k, q, x)
            if k < ORDER - 1:
                for j in range(q0 // 2, (q1 + 1) // 2):
                    apply_modes(wk[...], made, dst, 168, j)

    def take_levels(k, q, x):
        for c in range(3):
            total = lev[c, q] + F32(TABLE[c][k]) * x
            lev[c, q] = total
            if k == ORDER - 1:
                hi, lo = split(total)
                lv[c, 56 * q : 56 * q + 56, 0:128] = hi
                lv[c, 56 * q : 56 * q + 56, 128:256] = lo

    taylor_step(1, sb, 0, take_levels)

    @pl.when(core == 0)
    def _():
        pl.semaphore_wait(barrier, len(OTHERS))
        pl.semaphore_signal(met_sem.at[0], inc=1, device_id=partner_core, device_id_type=MESH)

    @pl.when(core == 1)
    def _():
        pl.semaphore_wait(met_sem.at[0], 1)

    requests = []
    for i in ASKED:
        requests.append(
            pltpu.make_async_remote_copy(
                src_ref=rq_send.at[i // 8],
                dst_ref=rq_recv.at[i],
                send_sem=rq_ssem.at[i],
                recv_sem=rq_rsem.at[i],
                device_id=(dom, origin(i)),
                device_id_type=MESH,
            )
        )
    for copy in requests:
        copy.start()
    copies = {}
    for i in range(RAW):
        copies[i] = pltpu.make_async_remote_copy(
            src_ref=raw_send.at[pl.ds(SHARE * i, SHARE)],
            dst_ref=raw_recv.at[pl.ds(SHARE * i, SHARE)],
            send_sem=ssem.at[i],
            recv_sem=rsem.at[i],
            device_id=(dom, peer(i)),
            device_id_type=MESH,
        )
        copies[i].start()
    loads["lown"].wait()

    for k in range(2, ORDER - 1):
        taylor_step(k, sb, 0, take_levels)

    @pl.when(core == 1)
    def _():
        pl.semaphore_wait(barrier, 4)
        pl.semaphore_signal(met_sem.at[1], inc=1, device_id=partner_core, device_id_type=MESH)

    @pl.when(core == 0)
    def _():
        pl.semaphore_wait(met_sem.at[1], 1)

    halo_requests = []
    for j, target in enumerate((below, above)):
        halo_requests.append(
            pltpu.make_async_remote_copy(
                src_ref=rq_send.at[2],
                dst_ref=rq_recv.at[N_GRP + j],
                send_sem=rq_ssem.at[N_GRP + j],
                recv_sem=rq_rsem.at[N_GRP + j],
                device_id=target,
                device_id_type=MESH,
            )
        )
    for copy in halo_requests:
        copy.start()
    loads["flag"].wait()

    taylor_step(ORDER - 1, sb, 0, take_levels)
    for c in range(3):
        lv[c, ROWS:WIRE, :] = jnp.zeros((WIRE - ROWS, 256), F32)
    for h in range(2):
        for c in range(3):
            picked[c, EARLY:320, 256 * h : 256 * h + 256] = dot_nt(
                sel[EARLY:320, :], lv[c, 256 * h : 256 * h + 256, :]
            )

    for copy in requests:
        copy.wait_recv()
    asked = rq_recv[0:N_GRP].reshape(N_GRP, 128)
    block = lax.broadcasted_iota(jnp.int32, (8, 128), 0)
    lane8 = lax.broadcasted_iota(jnp.int32, (8, 128), 1)
    rows = []
    for t in range(2):
        mine = jnp.where(block == lane8 // SHARE, asked[8 * t : 8 * t + 8], 0.0)
        rows.append(jnp.sum(mine, axis=0, keepdims=True))
    def fill(t, row, start, stop):
        span = pl.ds(128 * t + start, stop - start)
        col = jnp.transpose(jnp.broadcast_to(row, (128, 128)))[start:stop]
        is0 = col < 0.5
        is1 = col < 1.5
        for n in range(4):
            lanes = pl.ds(128 * n, 128)
            send[span, lanes] = jnp.where(
                is0, picked[0, span, lanes], jnp.where(is1, picked[1, span, lanes], picked[2, span, lanes])
            )

    fill(0, rows[0], EARLY, 128)
    fill(1, rows[1], 0, 128)

    for i in ASKED:
        copies[i] = pltpu.make_async_remote_copy(
            src_ref=send.at[pl.ds(SHARE * i, SHARE)],
            dst_ref=recv.at[pl.ds(SHARE * i, SHARE)],
            send_sem=ssem.at[i],
            recv_sem=rsem.at[i],
            device_id=(dom, peer(i)),
            device_id_type=MESH,
        )
    for i in copies:
        if i >= RAW:
            copies[i].start()
    recv[SHARE * SELF : SHARE * SELF + SHARE, :] = send[SHARE * SELF : SHARE * SELF + SHARE, :]

    for name in ("lacross", "riem", "pface", "coh", "relax"):
        loads[name].wait()

    for q in range(QUANT):
        x = jnp.where(ids == 0, lev[0, q], jnp.where(ids == 1, lev[1, q], lev[2, q]))
        store_operand(rs.at[0], q, x)
    for f in range(4):
        wpad[0, 0:56, 0:56] = lown[f]
        stack_weights(wpad[0, 0:56, :], wown, pl.ds(168 + 56 * f, 56))
    for j in range(5):
        apply_modes(wown[...], rs.at[0], kx.at[0], 392, j)

    def trace_terms(source, row0, side, f, acc, q0, q1):
        for p in range(QUANT):
            x = tiles(source[p, row0 : row0 + 56, :])
            for q in range(q0, q1):
                s = jnp.broadcast_to(riem[side, p, q, pl.ds(f, 1), :], (8, 128))
                acc[q] = acc[q] - x * s[None]

    for q0, q1 in QGROUPS:
        acc = {q: tiles(old[q]) for q in range(q0, q1)}
        for p in range(QUANT):
            for d in range(3):
                x = tiles(kx[0, p, 56 * d : 56 * d + 56, :])
                for q in range(q0, q1):
                    acc[q] = acc[q] + x * sb[(p * 9 + q) * 3 + d][None]
        for f in range(4):
            trace_terms(kx.at[0], 168 + 56 * f, 0, f, acc, q0, q1)
        for q in range(q0, q1):
            upd[q] = acc[q].reshape(56, 128)

    for copy in halo_requests:
        copy.wait_recv()
    from_above = jnp.broadcast_to(rq_recv[N_GRP], (8, 128))
    from_below = jnp.broadcast_to(rq_recv[N_GRP + 1], (8, 128))
    halo = jnp.where(
        lane8 < HALO, pltpu.roll(from_below, 128 - HALO, 1), pltpu.roll(from_above, HALO, 1)
    )
    fill(2, halo[0:1], 0, 64)
    for j, target in enumerate((below, above)):
        copies[N_GRP + j] = pltpu.make_async_remote_copy(
            src_ref=send.at[pl.ds(GRP_SLOTS + HALO * j, HALO)],
            dst_ref=recv.at[pl.ds(GRP_SLOTS + HALO * (1 - j), HALO)],
            send_sem=ssem.at[N_GRP + j],
            recv_sem=rsem.at[N_GRP + j],
            device_id=target,
            device_id_type=MESH,
        )
    for j in range(2):
        copies[N_GRP + j].start()
    for i in range(RAW):
        copies[i].wait_recv()

    ids2 = jnp.concatenate([ids, ids], axis=1)
    for half in range(2):
        m = qm[0:128, 256 * half : 256 * half + 256]
        total = None
        for c in range(3):
            mc = jnp.where(ids2 == c, m, 0.0)
            part = dot(lv[c], jnp.concatenate([mc, mc], axis=0))
            total = part if total is None else total + part
        near[2 * half] = total[:, 0:128]
        near[2 * half + 1] = total[:, 128:256]

    for f in range(4):
        for j in range(4):
            wpad[0, 0:56, 0:56] = lacross[f, j]
            stack_weights(wpad[0, 0:56, :], wx.at[f], pl.ds(56 * j, 56))

    raw_state[...] = jnp.transpose(raw_recv[...])
    for r in range(243):
        raw_sb[r] = jnp.broadcast_to(raw_state[pl.ds(WIRE + r, 1), :], (8, 128))
    level = rq_send[0]

    def weight(k):
        return jnp.where(level < 0.5, TABLE[0][k], jnp.where(level < 1.5, TABLE[1][k], TABLE[2][k]))

    def take_near(k, q, x):
        raw_near[56 * q : 56 * q + 56, :] = raw_near[56 * q : 56 * q + 56, :] + weight(k) * x

    for q in range(QUANT):
        x = raw_state[56 * q : 56 * q + 56, :]
        store_operand(rs.at[1], q, x)
        raw_near[56 * q : 56 * q + 56, :] = weight(0) * x
    raw_near[ROWS:WIRE, :] = jnp.zeros((WIRE - ROWS, 128), F32)
    for j in range(5):
        apply_modes(wk[...], rs.at[1], kx.at[1], 168, j)
    for k in range(1, ORDER):
        taylor_step(k, raw_sb, 1, take_near)

    def add_received(first, row0, extra):
        block = jnp.transpose(recv[first : first + 128, :])
        if extra is not None:
            block = block + extra
        hi, lo = split(block)
        lhs = jnp.concatenate([hi, lo], axis=1)
        for half in range(2):
            m = qm[row0 : row0 + 128, 256 * half : 256 * half + 256]
            part = dot(lhs, jnp.concatenate([m, m], axis=0))
            near[2 * half] = near[2 * half] + part[:, 0:128]
            near[2 * half + 1] = near[2 * half + 1] + part[:, 128:256]

    recv[320:384, :] = jnp.zeros((64, WIRE), F32)
    recv[0:EARLY, :] = jnp.zeros((EARLY, WIRE), F32)
    for j in range(2):
        copies[N_GRP + j].wait_recv()
    add_received(256, 384, None)
    for i in range(RAW, 8):
        if i != SELF:
            copies[i].wait_recv()
    add_received(0, 128, raw_near[...])
    for i in range(8, 16):
        copies[i].wait_recv()
    add_received(128, 256, None)

    for f in range(4):
        work = rs.at[f % 2]
        lifted = kx.at[f % 2]
        side = pface[pl.ds(f, 1), :]
        is0 = side == 0
        is1 = side == 1
        is2 = side == 2
        for q in range(QUANT):
            store_operand(work, q, near[f, 56 * q : 56 * q + 56, :])
        for j in range(5):
            apply_modes(wx[f], work, lifted, 224, j)
        for p in range(QUANT):
            parts = [lifted[p, 56 * j : 56 * j + 56, :] for j in range(4)]
            chosen[f % 2, p] = jnp.where(
                is0, parts[0], jnp.where(is1, parts[1], jnp.where(is2, parts[2], parts[3]))
            )
        for q0, q1 in QGROUPS:
            acc = {q: tiles(upd[q]) for q in range(q0, q1)}
            trace_terms(chosen.at[f % 2], 0, 1, f, acc, q0, q1)
            for q in range(q0, q1):
                upd[q] = acc[q].reshape(56, 128)

    first = [upd[q, 0:1, :] for q in range(6)]
    mean = (first[0] + first[1] + first[2]) / 3.0
    dev = [first[q] - mean if q < 3 else first[q] for q in range(6)]
    second = 0.5 * (dev[0] * dev[0] + dev[1] * dev[1] + dev[2] * dev[2])
    second = second + dev[3] * dev[3] + dev[4] * dev[4] + dev[5] * dev[5]
    strength = jnp.sqrt(second)
    limit = cohesion[...]
    excess = jnp.maximum(strength - limit, 0.0) / jnp.maximum(strength, limit)
    interval = jnp.where(ids == 0, base_step, jnp.where(ids == 1, 2.0 * base_step, 4.0 * base_step))
    factor = yflag[...].astype(F32) * excess * (1.0 - jnp.exp(-interval / relax_time[...]))
    pressure = (upd[0] + upd[1] + upd[2]) * F32(1.0 / 3.0)
    for q in range(QUANT):
        x = upd[q]
        if q < 3:
            out[q] = x - factor * (x - pressure)
        elif q < 6:
            out[q] = x - factor * x
        else:
            out[q] = x

    for copy in requests + halo_requests:
        copy.wait_send()
    for copy in copies.values():
        copy.wait_send()


def on_device(
    old_state,
    stiffness,
    jacobians,
    lift_own,
    lift_across,
    riemann,
    cluster_ids,
    send_slots,
    face_partner,
    partner_face,
    cohesion,
    relax_time,
    yield_flag,
):
    args = (
        old_state,
        stiffness,
        jnp.transpose(jacobians, (1, 2, 0, 3)),
        lift_own,
        lift_across,
        jnp.transpose(riemann, (0, 2, 3, 1, 4)),
        cluster_ids.reshape(1, ELEM),
        send_slots,
        face_partner,
        partner_face,
        cohesion.reshape(1, ELEM),
        relax_time.reshape(1, ELEM),
        yield_flag.reshape(1, ELEM),
    )
    args = tuple(pltpu.with_memory_space_constraint(a, pltpu.HBM) for a in args)
    sems = [pltpu.SemaphoreType.DMA((N_GRP + 2,)) for _ in range(4)]
    return pl.pallas_call(
        kernel,
        out_shape=jax.ShapeDtypeStruct((QUANT, MODES, ELEM), F32),
        in_specs=[pl.BlockSpec(memory_space=pltpu.HBM)] * len(args),
        out_specs=pl.BlockSpec(memory_space=pltpu.VMEM),
        scratch_shapes=[pltpu.VMEM(a.shape, a.dtype) for a in args]
        + [
            pltpu.VMEM((2, 256, 1152), F32),
            pltpu.VMEM((2, QUANT, 392, 128), F32),
            pltpu.VMEM((243, 8, 128), F32),
            pltpu.VMEM((3, 128, 128), F32),
            pltpu.VMEM((168, 256), F32),
            pltpu.VMEM((392, 256), F32),
            pltpu.VMEM((4, 224, 256), F32),
            pltpu.VMEM((512, 512), F32),
            pltpu.VMEM((3, QUANT, MODES, 128), F32),
            pltpu.VMEM((3, WIRE, 256), F32),
            pltpu.VMEM((320, 256), F32),
            pltpu.VMEM((3, 320, WIRE), F32),
            pltpu.VMEM((4, WIRE, 128), F32),
            pltpu.VMEM((2, QUANT, MODES, 128), F32),
            pltpu.VMEM((QUANT, MODES, 128), F32),
            pltpu.VMEM((320, WIRE), F32),
            pltpu.VMEM((384, WIRE), F32),
            pltpu.VMEM((RAW_WIRE, 256), F32),
            pltpu.VMEM((EARLY, RAW_WIRE), F32),
            pltpu.VMEM((128, RAW_WIRE), F32),
            pltpu.VMEM((RAW_WIRE, 128), F32),
            pltpu.VMEM((243, 8, 128), F32),
            pltpu.VMEM((WIRE, 128), F32),
            pltpu.VMEM((3, 1, 128), F32),
            pltpu.VMEM((N_GRP + 2, 1, 128), F32),
            pltpu.SemaphoreType.DMA((13,)),
        ]
        + sems
        + [pltpu.SemaphoreType.REGULAR((2,))],
        compiler_params=pltpu.CompilerParams(
            collective_id=0, has_side_effects=True, vmem_limit_bytes=40 * 1024 * 1024
        ),
    )(*args)


def solution(mesh):
    in_specs = (
        P(None, None, ("dom", "grp")),
        P(),
        P(None, None, None, ("dom", "grp")),
        P(),
        P(),
        P(None, None, None, None, ("dom", "grp")),
        P(("dom", "grp")),
        P(("dom", "grp")),
        P(None, ("dom", "grp")),
        P(None, ("dom", "grp")),
        P(("dom", "grp")),
        P(("dom", "grp")),
        P(("dom", "grp")),
    )
    out_specs = P(None, None, ("dom", "grp"))
    return jax.shard_map(
        on_device, mesh=mesh, in_specs=in_specs, out_specs=out_specs, check_vma=False
    )
```
